32 devices in a mesh: rep: 4 (over x, y), dp: 8 (over z, core).
Axes of the slice: x: 2, y: 2, z: 4, core: 2. Of those that a mesh axis runs over, the one named last changes fastest.
Arguments:
- x: bfloat16 [32, 1024, 512], P(('rep', 'dp')), parts along dimension 0
- dy: bfloat16 [32, 1024, 512], P(('rep', 'dp')), parts along dimension 0
- w_gate: bfloat16 [2, 512, 8192], P(None, 'dp')
- w_up: bfloat16 [2, 512, 8192], P(None, 'dp')
- w_down: bfloat16 [2, 8192, 512], P(None, 'dp')
Outputs:
- output 1: bfloat16 [32, 1024, 512], P(('rep', 'dp')), parts along dimension 0
- output 2: bfloat16 [8, 512, 8192], P('rep', 'dp'), parts along dimension 0
- output 3: bfloat16 [8, 512, 8192], P('rep', 'dp'), parts along dimension 0
- output 4: bfloat16 [8, 8192, 512], P('rep', 'dp'), parts along dimension 0
There are 4 independent parts. The reference program is written for one: setup_inputs(seed, part) draws one part's arguments, and reference() takes and returns one part's arrays. A program takes and returns all parts, laid end to end along the dimension named above; an argument that names none is the same for every part.
All inputs are finite; a program needn't handle non-finite values.
Results may differ from the reference program's by a relative error of at most 0.018.
Values are sent between devices in bfloat16 or wider.
A program may use at most 2 GiB of HBM per device.

```python
import jax
import jax.numpy as jnp
from jax import lax

SEQUENCES = 8
TOKENS = 1024
D = 512
FF = 8192
LAYERS = 2
NAMES = ("w_gate", "w_up", "w_down")
SHAPES = {"w_gate": (LAYERS, D, FF), "w_up": (LAYERS, D, FF), "w_down": (LAYERS, FF, D)}


def bump(key, n, height):
    away = (jnp.arange(n, dtype=jnp.int32) - jax.random.randint(key, (), 0, n, jnp.int32)) % n
    return jnp.where(away < n // 8, height, 1.0)


def together(key, own, strength):
    shared = jax.random.normal(key, own.shape[1:], jnp.float32)
    return (own + strength * shared) * lax.rsqrt(1 + strength * strength)


def setup_inputs(seed: int = 0, part: int = 0) -> dict:
    kx, kdy, ka, kb, kz, kf, kh, kl, *kw = jax.random.split(jax.random.key(seed), 8 + len(NAMES))
    kx, kdy, ka, kb = (jax.random.fold_in(k, part) for k in (kx, kdy, ka, kb))
    shape = (SEQUENCES, TOKENS, D)
    much_x, much_dy = jax.random.uniform(kz, (2,), jnp.float32, 0.0, 1.0)
    layers = 2.0 ** jax.random.uniform(kl, (LAYERS, 1, 1), jnp.float32, -1.0, 1.0)
    x = together(ka, jax.random.normal(kx, shape, jnp.float32), much_x) * bump(kf, D, 4.0)
    dy = together(kb, jax.random.normal(kdy, shape, jnp.float32), much_dy)
    drawn = {"x": x.astype(jnp.bfloat16), "dy": (dy * (SEQUENCES * TOKENS) ** -0.5).astype(jnp.bfloat16)}
    for key, name in zip(kw, NAMES, strict=True):
        w = jax.random.normal(key, SHAPES[name], jnp.float32) * SHAPES[name][1] ** -0.5
        drawn[name] = (w * {"w_gate": 1.0, "w_up": bump(kh, FF, 4.0), "w_down": layers}[name]).astype(jnp.bfloat16)
    return drawn


def matmul(a, w):
    return jnp.dot(a, w, preferred_element_type=jnp.float32).astype(jnp.bfloat16)


def normed(h):
    wide = h.astype(jnp.float32)
    scale = lax.rsqrt(jnp.mean(wide**2, -1, keepdims=True) + 1e-6)
    return (wide * scale).astype(jnp.bfloat16)


def layer(h, w):
    a = normed(h)
    gate = jnp.dot(a, w["w_gate"], preferred_element_type=jnp.float32)
    up = jnp.dot(a, w["w_up"], preferred_element_type=jnp.float32)
    return h + matmul((jax.nn.silu(gate) * up).astype(jnp.bfloat16), w["w_down"])


def stack(weights, h):
    return lax.scan(lambda h, w: (layer(h, w), None), h, weights)[0]


def reference(x, dy, w_gate, w_up, w_down):
    weights = dict(zip(NAMES, (w_gate, w_up, w_down), strict=True))

    def take(so_far, sequence):
        h, by_y = sequence
        _, back = jax.vjp(stack, weights, h)
        by_weights, by_h = back(by_y)
        return jax.tree.map(lambda total, term: total + term.astype(jnp.float32), so_far, by_weights), by_h

    none_yet = {name: jnp.zeros(w.shape, jnp.float32) for name, w in weights.items()}
    by_weights, by_x = lax.scan(take, none_yet, (x, dy))
    return (by_x, *(by_weights[name].astype(jnp.bfloat16) for name in NAMES))
```

```python
import functools

import jax
import jax.numpy as jnp
from jax import lax
from jax.sharding import PartitionSpec as P

F32, BF16 = jnp.float32, jnp.bfloat16


def normed(h):
    wide = h.astype(F32)
    scale = lax.rsqrt(jnp.mean(wide**2, -1, keepdims=True) + 1e-6)
    return (wide * scale).astype(BF16)


def dot(a, b, ca, cb):
    return lax.dot_general(a, b, (((ca,), (cb,)), ((), ())), preferred_element_type=F32)


def norm_back(h, da):
    wide = h.astype(F32)
    scale = lax.rsqrt(jnp.mean(wide**2, -1, keepdims=True) + 1e-6)
    da = da.astype(F32)
    inner = jnp.sum(da * wide, -1, keepdims=True)
    return (da * scale - wide * (scale**3 * inner / h.shape[-1])).astype(BF16)


def forward(h, a, wg, wu, wd):
    gate, up = dot(a, wg, 1, 0), dot(a, wu, 1, 0)
    p = (jax.nn.silu(gate) * up).astype(BF16)
    return h + dot(p, wd, 1, 0).astype(BF16)


def hidden_back(a, g, wg, wu, wd):
    gate, up = dot(a, wg, 1, 0), dot(a, wu, 1, 0)
    dp = dot(g, wd, 1, 1).astype(BF16).astype(F32)
    sig = jax.nn.sigmoid(gate)
    s = gate * sig
    p = (s * up).astype(BF16)
    dup = (dp * s).astype(BF16)
    dgate = (dp * up * (sig + s * (1 - sig))).astype(BF16)
    return p, dgate, dup


def back(h, a, g, wg, wu, wd):
    _, dgate, dup = hidden_back(a, g, wg, wu, wd)
    da = dot(dgate, wg, 1, 1).astype(BF16) + dot(dup, wu, 1, 1).astype(BF16)
    return g + norm_back(h, da)


def weights_back(a, g, wg, wu, wd):
    p, dgate, dup = hidden_back(a, g, wg, wu, wd)
    return dot(a, dgate, 0, 0).astype(BF16), dot(a, dup, 0, 0).astype(BF16), dot(p, g, 0, 0).astype(BF16)


def solution(mesh):
    layers = 2

    def body(x, dy, wg, wu, wd):
        gather = functools.partial(lax.all_gather, axis_name="dp", axis=0, tiled=True)
        me = lax.axis_index("dp")
        h, g = x[0], dy[0]
        width = wd.shape[1]
        full = [(gather(wg[n]), gather(wu[n]), gather(wd[n])) for n in range(layers)]
        own = [(lax.dynamic_slice_in_dim(f[0], me * width, width, 1), lax.dynamic_slice_in_dim(f[1], me * width, width, 1), wd[n])
               for n, f in enumerate(full)]
        hs, acts, all_a = [], [], []
        for n in range(layers):
            a = normed(h)
            hs.append(h)
            acts.append(a)
            all_a.append(gather(a))
            if n < layers - 1:
                h = forward(h, a, *full[n])
        grads = [None] * layers
        for n in reversed(range(layers)):
            all_g = gather(g)
            g = back(hs[n], acts[n], g, *full[n])
            bg, bu, bd = weights_back(all_a[n], all_g, *own[n])
            bg, bu = (lax.all_to_all(t, "dp", 0, 1, tiled=True) for t in (bg, bu))
            grads[n] = (bg, bu, bd)
        return (g[None], *(jnp.stack(t) for t in zip(*grads)))

    rows = P(("rep", "dp"), None, None)
    w = P(None, "dp", None)
    out = P("rep", "dp", None)
    return jax.shard_map(body, mesh=mesh, in_specs=(rows, rows, w, w, w), out_specs=(rows, out, out, out), check_vma=False)
```

```python
import functools

import jax
import jax.numpy as jnp
from jax import lax
from jax.experimental import pallas as pl
from jax.experimental.pallas import tpu as pltpu
from jax.sharding import PartitionSpec as P

F32, BF16 = jnp.float32, jnp.bfloat16


def normed(h):
    wide = h.astype(F32)
    scale = lax.rsqrt(jnp.mean(wide**2, -1, keepdims=True) + 1e-6)
    return (wide * scale).astype(BF16)


def dot(a, b, ca, cb):
    return lax.dot_general(a, b, (((ca,), (cb,)), ((), ())), preferred_element_type=F32)


def norm_back(h, da):
    wide = h.astype(F32)
    scale = lax.rsqrt(jnp.mean(wide**2, -1, keepdims=True) + 1e-6)
    da = da.astype(F32)
    inner = jnp.sum(da * wide, -1, keepdims=True)
    return (da * scale - wide * (scale**3 * inner / h.shape[-1])).astype(BF16)


def hidden_back(gate, up, dp):
    dp = dp.astype(BF16).astype(F32)
    sig = jax.nn.sigmoid(gate)
    s = gate * sig
    return (s * up).astype(BF16), (dp * up * (sig + s * (1 - sig))).astype(BF16), (dp * s).astype(BF16)


ROWS = 256


def forward_kernel(h_ref, wg_ref, wu_ref, wd_ref, out_ref, normed_ref, a_ref, acc_ref):
    step = pl.program_id(0)

    @pl.when(step == 0)
    def _():
        a_ref[...] = normed(h_ref[...])
        acc_ref[...] = jnp.zeros_like(acc_ref)

    for r in range(0, h_ref.shape[0], ROWS):
        rows = pl.ds(r, ROWS)
        a = a_ref[rows, :]
        gate, up = dot(a, wg_ref[...], 1, 0), dot(a, wu_ref[...], 1, 0)
        p = (gate * jax.nn.sigmoid(gate) * up).astype(BF16)
        acc_ref[rows, :] += dot(p, wd_ref[...], 1, 0)

    @pl.when(step == pl.num_programs(0) - 1)
    def _():
        h = h_ref[...] + acc_ref[...].astype(BF16)
        out_ref[...] = h
        normed_ref[...] = normed(h)


def forward(h, wg, wu, wd, width=1024):
    tokens, d = h.shape
    ff = wd.shape[0]
    whole = pl.BlockSpec((tokens, d), lambda k: (0, 0))
    column = pl.BlockSpec((d, width), lambda k: (0, k))
    return pl.pallas_call(
        forward_kernel,
        grid=(ff // width,),
        in_specs=[whole, column, column, pl.BlockSpec((width, d), lambda k: (k, 0))],
        out_specs=[whole, whole],
        out_shape=[jax.ShapeDtypeStruct(h.shape, BF16)] * 2,
        scratch_shapes=[pltpu.VMEM((tokens, d), BF16), pltpu.VMEM((tokens, d), F32)],
        cost_estimate=pl.CostEstimate(flops=6 * tokens * d * ff, bytes_accessed=6 * d * ff, transcendentals=tokens * ff),
        name="forward",
    )(h, wg, wu, wd)


def back_kernel(h_ref, g_ref, wg_ref, wu_ref, wd_ref, out_ref, a_ref, accg_ref, accu_ref):
    step = pl.program_id(0)

    @pl.when(step == 0)
    def _():
        a_ref[...] = normed(h_ref[...])
        accg_ref[...] = jnp.zeros_like(accg_ref)
        accu_ref[...] = jnp.zeros_like(accu_ref)

    for r in range(0, h_ref.shape[0], ROWS):
        rows = pl.ds(r, ROWS)
        a = a_ref[rows, :]
        gate, up = dot(a, wg_ref[...], 1, 0), dot(a, wu_ref[...], 1, 0)
        _, dgate, dup = hidden_back(gate, up, dot(g_ref[rows, :], wd_ref[...], 1, 1))
        accg_ref[rows, :] += dot(dgate, wg_ref[...], 1, 1)
        accu_ref[rows, :] += dot(dup, wu_ref[...], 1, 1)

    @pl.when(step == pl.num_programs(0) - 1)
    def _():
        da = accg_ref[...].astype(BF16) + accu_ref[...].astype(BF16)
        out_ref[...] = g_ref[...] + norm_back(h_ref[...], da)


def back(h, g, wg, wu, wd, width=1024):
    tokens, d = h.shape
    ff = wd.shape[0]
    whole = pl.BlockSpec((tokens, d), lambda k: (0, 0))
    column = pl.BlockSpec((d, width), lambda k: (0, k))
    return pl.pallas_call(
        back_kernel,
        grid=(ff // width,),
        in_specs=[whole, whole, column, column, pl.BlockSpec((width, d), lambda k: (k, 0))],
        out_specs=whole,
        out_shape=jax.ShapeDtypeStruct(h.shape, BF16),
        scratch_shapes=[pltpu.VMEM((tokens, d), BF16), pltpu.VMEM((tokens, d), F32), pltpu.VMEM((tokens, d), F32)],
        cost_estimate=pl.CostEstimate(flops=10 * tokens * d * ff, bytes_accessed=6 * d * ff, transcendentals=tokens * ff),
        name="back",
    )(h, g, wg, wu, wd)


GROUP = 8


def weights_kernel(a_ref, g_ref, wg_ref, wu_ref, wd_ref, bg_ref, bu_ref, bd_ref, accg_ref, accu_ref, accd_ref, stageg_ref, stageu_ref,
                   kept, sends, receives):
    chunk, step = pl.program_id(0), pl.program_id(1)
    chunks, steps = pl.num_programs(0), pl.num_programs(1)
    tokens, width = a_ref.shape[0], wg_ref.shape[1]
    height = bg_ref.shape[0]
    rep, me = lax.axis_index("rep"), lax.axis_index("dp")
    barrier = pltpu.get_barrier_semaphore()

    @pl.when((chunk == 0) & (step == 0))
    def _():
        for j in range(1, GROUP):
            pl.semaphore_signal(barrier, inc=1, device_id=(rep, lax.rem(me + j, GROUP)), device_id_type=pl.DeviceIdType.MESH)

    @pl.when(step == 0)
    def _():
        for acc in (accg_ref, accu_ref, accd_ref):
            acc[...] = jnp.zeros_like(acc)

    ps, dgs, dus = [], [], []
    for r in range(0, tokens, ROWS):
        rows = pl.ds(r, ROWS)
        a, g = a_ref[rows, :], g_ref[rows, :]
        gate, up = dot(a, wg_ref[...], 1, 0), dot(a, wu_ref[...], 1, 0)
        p, dgate, dup = hidden_back(gate, up, dot(g, wd_ref[...], 1, 1))
        ps.append(p), dgs.append(dgate), dus.append(dup)
    p, dgate, dup = (jnp.concatenate(t, 0) for t in (ps, dgs, dus))
    accg_ref[...] += dot(a_ref[...], dgate, 0, 0)
    accu_ref[...] += dot(a_ref[...], dup, 0, 0)
    accd_ref[...] += dot(p, g_ref[...], 0, 0)

    pairs = ((stageg_ref, bg_ref), (stageu_ref, bu_ref))

    def to_own(c, m):
        stage, out = pairs[m]
        columns = pl.ds(pl.multiple_of((me * chunks + c) * width, width), width)
        return pltpu.make_async_copy(stage.at[c, pl.ds(pl.multiple_of(me * height, height), height)], out.at[:, columns], kept.at[c, m])

    def to_peer(c, m, j):
        stage, out = pairs[m]
        columns = pl.ds(pl.multiple_of((me * chunks + c) * width, width), width)
        peer = lax.rem(me + j, GROUP)
        return pltpu.make_async_remote_copy(
            src_ref=stage.at[c, pl.ds(pl.multiple_of(peer * height, height), height)], dst_ref=out.at[:, columns],
            send_sem=sends.at[c, m, j - 1], recv_sem=receives.at[c, m, j - 1], device_id=(rep, peer), device_id_type=pl.DeviceIdType.MESH)

    @pl.when((chunk == 0) & (step == steps - 1))
    def _():
        pl.semaphore_wait(barrier, GROUP - 1)

    @pl.when(step == steps - 1)
    def _():
        for m, acc in ((0, accg_ref), (1, accu_ref)):
            pairs[m][0][chunk] = acc[...].astype(BF16)
            for j in (4, 3, 5, 2, 6, 1, 7):
                to_peer(chunk, m, j).start()
            to_own(chunk, m).start()
        bd_ref[...] = accd_ref[...].astype(BF16)

    @pl.when((chunk == chunks - 1) & (step == steps - 1))
    def _():
        def finish(c, _):
            for m in range(2):
                to_own(c, m).wait()
                for j in range(1, GROUP):
                    to_peer(c, m, j).wait()
            return 0

        lax.fori_loop(0, chunks, finish, 0)


def weights_back(a, g, wg, wu, wd, collective_id, width=256, block=1024):
    tokens, d = a.shape
    ff = wd.shape[0]
    chunks = ff // width
    rows = pl.BlockSpec((block, d), lambda k, t: (t, 0))
    column = pl.BlockSpec((d, width), lambda k, t: (0, k))
    down = pl.BlockSpec((width, d), lambda k, t: (k, 0))
    anywhere = pl.BlockSpec(memory_space=pltpu.HBM)
    spread = jax.ShapeDtypeStruct((d // GROUP, ff * GROUP), BF16)
    dma = pltpu.SemaphoreType.DMA
    return pl.pallas_call(
        weights_kernel,
        grid=(chunks, tokens // block),
        in_specs=[rows, rows, column, column, down],
        out_specs=[anywhere, anywhere, down],
        out_shape=[spread, spread, jax.ShapeDtypeStruct((ff, d), BF16)],
        scratch_shapes=[pltpu.VMEM((d, width), F32), pltpu.VMEM((d, width), F32), pltpu.VMEM((width, d), F32),
                        pltpu.VMEM((chunks, d, width), BF16), pltpu.VMEM((chunks, d, width), BF16),
                        dma((chunks, 2)), dma((chunks, 2, GROUP - 1)), dma((chunks, 2, GROUP - 1))],
        compiler_params=pltpu.CompilerParams(collective_id=collective_id, has_side_effects=True),
        cost_estimate=pl.CostEstimate(flops=12 * tokens * d * ff, bytes_accessed=4 * d * tokens * chunks, transcendentals=tokens * ff),
        name="weights_back",
    )(a, g, wg, wu, wd)


MESH = pl.DeviceIdType.MESH


class Gather:
    def __init__(self, n, own, out, stage, load, store, zs, zr, hs, ps, pr, fs, fr, cs, cr):
        self.n, self.own, self.out, self.stage = n, own, out, stage
        self.load, self.store = load, store
        self.zs, self.zr, self.hs, self.ps, self.pr, self.fs, self.fr, self.cs, self.cr = zs, zr, hs, ps, pr, fs, fr, cs, cr
        rep, dp = lax.axis_index("rep"), lax.axis_index("dp")
        z, core = dp // 2, lax.rem(dp, 2)
        self.rep, self.dp, self.z, self.core = rep, dp, z, core
        self.inner = lax.rem((z + 1) // 2, 2)
        self.high = z // 2
        self.over_x = lax.rem(rep + 2, 4)
        self.over_y = rep + 1 - 2 * lax.rem(rep, 2)
        self.across = 3 - rep
        self.to_x, self.to_y, self.to_core = (self.over_x, dp), (self.over_y, dp), (rep, z * 2 + 1 - core)
        self.sent, self.handed = [], []

    def along(self, z):
        return (self.rep, z * 2 + self.core)

    def source(self, k):
        low = (1 - self.z, 2, 3)[k]
        high = (5 - self.z, 1, 0)[k]
        return self.high * high + (1 - self.high) * low

    def barrier(self):
        semaphore = pltpu.get_barrier_semaphore()
        peers = [self.along(lax.rem(self.z + j, 4)) for j in (1, 2, 3)] + [self.to_x, self.to_y, self.to_core]
        for peer in peers:
            pl.semaphore_signal(semaphore, inc=1, device_id=peer, device_id_type=MESH)
        pl.semaphore_wait(semaphore, len(peers))

    def rows(self, i, z, core, quarter=None):
        size = self.own[i].shape[0]
        start = (z * 2 + core) * size
        if quarter is None:
            return self.out[i].at[pl.ds(pl.multiple_of(start, size), size)]
        part = size // 4
        return self.out[i].at[pl.ds(pl.multiple_of(start + quarter * part, part), part)]

    def copy(self, src, dst, send, receive, peer):
        return pltpu.make_async_remote_copy(src_ref=src, dst_ref=dst, send_sem=send, recv_sem=receive, device_id=peer, device_id_type=MESH)

    def start(self, *args):
        copy = self.copy(*args)
        copy.start()
        self.sent.append(copy)

    def begin(self, i):
        part = self.own[i].shape[0] // 4
        mine = self.own[i].at[pl.ds(pl.multiple_of(self.rep * part, part), part)]
        there = self.rows(i, self.z, self.core, self.rep)
        inner = self.inner
        outward = inner * (3 * self.z - 3) + (1 - inner) * (2 - self.z // 3)
        self.start(mine, there, self.zs.at[2 * i], self.zr.at[3 * i + inner], self.along(1 + lax.rem(self.z, 2)))
        self.start(mine, there, self.zs.at[2 * i + 1], self.zr.at[3 * i + 2 * (1 - inner)], self.along(outward))
        self.start(self.own[i], self.rows(i, self.z, self.core), self.cs.at[4 * i], self.cr.at[4 * i], self.to_core)
        self.local(i, 0).start()

    def local(self, i, leg):
        if leg == 0:
            return pltpu.make_async_copy(self.own[i], self.stage[i], self.load.at[i])
        return pltpu.make_async_copy(self.stage[i], self.rows(i, self.z, self.core), self.store.at[i])

    def keep(self, i):
        self.local(i, 0).wait()
        self.local(i, 1).start()

    def arrived(self, i, k, quarter, semaphore):
        ref = self.rows(i, self.source(k), self.core, quarter)
        self.copy(ref, ref, self.ps.at[0], semaphore, self.to_x).wait_recv()
        return ref

    def plane(self, i, k):
        at = 3 * i + k
        ref = self.arrived(i, k, self.rep, self.zr.at[at])
        if k:
            hand = self.copy(ref, ref, self.hs.at[2 * i + k - 1], self.zr.at[at], self.along(3 * self.high))
            pl.when(self.inner == 1)(hand.start)
            self.handed.append(hand)
        self.start(ref, ref, self.ps.at[2 * at], self.pr.at[2 * at], self.to_x)
        self.start(ref, ref, self.ps.at[2 * at + 1], self.pr.at[2 * at + 1], self.to_y)

    def diagonal(self, i, k):
        at = 3 * i + k
        from_x = self.arrived(i, k, self.over_x, self.pr.at[2 * at])
        from_y = self.arrived(i, k, self.over_y, self.pr.at[2 * at + 1])
        if at % 2:
            self.start(from_x, from_x, self.fs.at[at], self.fr.at[at], self.to_y)
        else:
            self.start(from_y, from_y, self.fs.at[at], self.fr.at[at], self.to_x)

    def share(self, i, k):
        self.arrived(i, k, self.across, self.fr.at[3 * i + k])
        ref = self.rows(i, self.source(k), self.core)
        self.start(ref, ref, self.cs.at[4 * i + k + 1], self.cr.at[4 * i + k + 1], self.to_core)

    def shared(self, i):
        for k in range(4):
            ref = self.rows(i, self.source(k - 1) if k else self.z, 1 - self.core)
            self.copy(ref, ref, self.ps.at[0], self.cr.at[4 * i + k], self.to_core).wait_recv()
        self.local(i, 1).wait()

    def steps(self, lag=2):
        items = [(i, k) for i in range(self.n) for k in range(3)]
        for step in range(len(items) + 2 * lag):
            if step < len(items):
                self.plane(*items[step])
            if lag <= step < len(items) + lag:
                self.diagonal(*items[step - lag])
            if 2 * lag <= step:
                self.share(*items[step - 2 * lag])
            yield step

    def finish(self):
        for copy in self.sent:
            copy.wait_send()
        for hand in self.handed:
            pl.when(self.inner == 1)(hand.wait_send)

    @staticmethod
    def scratch(blocks):
        n, dma = len(blocks), pltpu.SemaphoreType.DMA
        sizes = (n, n, 2 * n, 3 * n, 2 * n, 6 * n, 6 * n, 3 * n, 3 * n, 4 * n, 4 * n)
        return [pltpu.VMEM(b.shape, b.dtype) for b in blocks] + [dma((s,)) for s in sizes]


def gather_kernel(n, *refs):
    g = Gather(n, refs[:n], refs[n:2 * n], refs[2 * n:3 * n], *refs[3 * n:])
    g.barrier()
    for i in range(n):
        g.begin(i)
    for i in range(n):
        g.keep(i)
    for _ in g.steps():
        pass
    for i in range(n):
        g.shared(i)
    g.finish()


def gather(blocks, collective_id=0):
    n = len(blocks)
    anywhere = pl.BlockSpec(memory_space=pltpu.HBM)
    return pl.pallas_call(
        functools.partial(gather_kernel, n),
        in_specs=[anywhere] * n,
        out_specs=[anywhere] * n,
        out_shape=[jax.ShapeDtypeStruct((8 * b.shape[0], b.shape[1]), b.dtype) for b in blocks],
        scratch_shapes=Gather.scratch(blocks),
        compiler_params=pltpu.CompilerParams(collective_id=collective_id, has_side_effects=True),
        cost_estimate=pl.CostEstimate(flops=25_000_000_000 * n, bytes_accessed=48 * 2**20, transcendentals=0),
        name="gather",
    )(*blocks)


def solution(mesh):
    def body(x, dy, wg, wu, wd):
        gather_all = functools.partial(lax.all_gather, axis_name="dp", axis=0, tiled=True)
        me = lax.axis_index("dp")
        h0, g2 = x[0], dy[0]
        width = wd.shape[1]
        all_g2, all_a0 = gather_all(g2), gather_all(normed(h0))
        flat = gather([w[n] for n in range(2) for w in (wg, wu, wd)])
        full = flat[:3], flat[3:]
        own = [(*(lax.dynamic_slice_in_dim(w, me * width, width, 1) for w in f[:2]), wd[n]) for n, f in enumerate(full)]
        h0, all_g2, all_a0 = lax.optimization_barrier((h0, all_g2, all_a0))
        h1, a1 = forward(h0, *full[0])
        all_a1 = gather_all(a1)
        g1 = back(h1, g2, *full[1])
        all_g1 = gather_all(g1)
        g0 = back(h0, g1, *full[0])
        all_a1, g0 = lax.optimization_barrier((all_a1, g0))
        upper = weights_back(all_a1, all_g2, *own[1], collective_id=2)
        all_g1, upper = lax.optimization_barrier((all_g1, upper))
        lower = weights_back(all_a0, all_g1, *own[0], collective_id=2)
        return (g0[None], *(jnp.stack(t) for t in zip(lower, upper)))

    rows = P(("rep", "dp"), None, None)
    w = P(None, "dp", None)
    out = P("rep", "dp", None)
    return jax.shard_map(body, mesh=mesh, in_specs=(rows, rows, w, w, w), out_specs=(rows, out, out, out), check_vma=False)
```

```python
import functools

import jax
import jax.numpy as jnp
from jax import lax
from jax.experimental import pallas as pl
from jax.experimental.pallas import tpu as pltpu
from jax.sharding import PartitionSpec as P

F32, BF16 = jnp.float32, jnp.bfloat16


def normed(h):
    wide = h.astype(F32)
    scale = lax.rsqrt(jnp.mean(wide**2, -1, keepdims=True) + 1e-6)
    return (wide * scale).astype(BF16)


def dot(a, b, ca, cb):
    return lax.dot_general(a, b, (((ca,), (cb,)), ((), ())), preferred_element_type=F32)


def norm_back(h, da):
    wide = h.astype(F32)
    scale = lax.rsqrt(jnp.mean(wide**2, -1, keepdims=True) + 1e-6)
    da = da.astype(F32)
    inner = jnp.sum(da * wide, -1, keepdims=True)
    return (da * scale - wide * (scale**3 * inner / h.shape[-1])).astype(BF16)


def hidden_back(gate, up, dp):
    dp = dp.astype(BF16).astype(F32)
    sig = jax.nn.sigmoid(gate)
    s = gate * sig
    return (s * up).astype(BF16), (dp * up * (sig + s * (1 - sig))).astype(BF16), (dp * s).astype(BF16)


ROWS = 512


def back_kernel(h_ref, g_ref, wg_ref, wu_ref, wd_ref, out_ref, a_ref, accg_ref, accu_ref):
    step = pl.program_id(0)

    @pl.when(step == 0)
    def _():
        a_ref[...] = normed(h_ref[...])
        accg_ref[...] = jnp.zeros_like(accg_ref)
        accu_ref[...] = jnp.zeros_like(accu_ref)

    for r in range(0, h_ref.shape[0], ROWS):
        rows = pl.ds(r, ROWS)
        a = a_ref[rows, :]
        gate, up = dot(a, wg_ref[...], 1, 0), dot(a, wu_ref[...], 1, 0)
        _, dgate, dup = hidden_back(gate, up, dot(g_ref[rows, :], wd_ref[...], 1, 1))
        accg_ref[rows, :] += dot(dgate, wg_ref[...], 1, 1)
        accu_ref[rows, :] += dot(dup, wu_ref[...], 1, 1)

    @pl.when(step == pl.num_programs(0) - 1)
    def _():
        da = accg_ref[...].astype(BF16) + accu_ref[...].astype(BF16)
        out_ref[...] = g_ref[...] + norm_back(h_ref[...], da)


def back(h, g, wg, wu, wd, width=1024):
    tokens, d = h.shape
    ff = wd.shape[0]
    whole = pl.BlockSpec((tokens, d), lambda k: (0, 0))
    column = pl.BlockSpec((d, width), lambda k: (0, k))
    return pl.pallas_call(
        back_kernel,
        grid=(ff // width,),
        in_specs=[whole, whole, column, column, pl.BlockSpec((width, d), lambda k: (k, 0))],
        out_specs=whole,
        out_shape=jax.ShapeDtypeStruct(h.shape, BF16),
        scratch_shapes=[pltpu.VMEM((tokens, d), BF16), pltpu.VMEM((tokens, d), F32), pltpu.VMEM((tokens, d), F32)],
        cost_estimate=pl.CostEstimate(flops=10 * tokens * d * ff, bytes_accessed=6 * d * ff, transcendentals=tokens * ff),
        name="back",
    )(h, g, wg, wu, wd)


GROUP = 8


def weights_step(a_ref, g_ref, wg_ref, wu_ref, wd_ref, accg_ref, accu_ref, accd_ref):
    @pl.when(pl.program_id(1) == 0)
    def _():
        for acc in (accg_ref, accu_ref, accd_ref):
            acc[...] = jnp.zeros_like(acc)

    ps, dgs, dus = [], [], []
    for r in range(0, a_ref.shape[0], ROWS):
        rows = pl.ds(r, ROWS)
        a, g = a_ref[rows, :], g_ref[rows, :]
        gate, up = dot(a, wg_ref[...], 1, 0), dot(a, wu_ref[...], 1, 0)
        p, dgate, dup = hidden_back(gate, up, dot(g, wd_ref[...], 1, 1))
        ps.append(p), dgs.append(dgate), dus.append(dup)
    p, dgate, dup = (jnp.concatenate(t, 0) for t in (ps, dgs, dus))
    accg_ref[...] += dot(a_ref[...], dgate, 0, 0)
    accu_ref[...] += dot(a_ref[...], dup, 0, 0)
    accd_ref[...] += dot(p, g_ref[...], 0, 0)


def upper_kernel(a_ref, g_ref, wg_ref, wu_ref, wd_ref, bg_ref, bu_ref, bd_ref, *accs):
    weights_step(a_ref, g_ref, wg_ref, wu_ref, wd_ref, *accs)

    @pl.when(pl.program_id(1) == pl.num_programs(1) - 1)
    def _():
        for out, acc in zip((bg_ref, bu_ref, bd_ref), accs):
            out[...] = acc[...].astype(BF16)


def lower_kernel(a_ref, g_ref, wg_ref, wu_ref, wd_ref, ready_g, ready_u, bg_ref, bu_ref, bd_ref, cg_ref, cu_ref,
                 accg_ref, accu_ref, accd_ref, stageg_ref, stageu_ref, kept, sends, receives):
    chunk, step = pl.program_id(0), pl.program_id(1)
    chunks, steps = pl.num_programs(0), pl.num_programs(1)
    width = wg_ref.shape[1]
    height = bg_ref.shape[0]
    rep, me = lax.axis_index("rep"), lax.axis_index("dp")
    barrier = pltpu.get_barrier_semaphore()

    @pl.when((chunk == 0) & (step == 0))
    def _():
        for j in range(1, GROUP):
            pl.semaphore_signal(barrier, inc=1, device_id=(rep, lax.rem(me + j, GROUP)), device_id_type=pl.DeviceIdType.MESH)

    weights_step(a_ref, g_ref, wg_ref, wu_ref, wd_ref, accg_ref, accu_ref, accd_ref)

    def place(c, m):
        if isinstance(c, int) and c < 0:
            return ((ready_g, cg_ref), (ready_u, cu_ref))[m], pl.ds(pl.multiple_of(me * chunks * width, chunks * width), chunks * width), 0
        stage, out = ((stageg_ref, bg_ref), (stageu_ref, bu_ref))[m]
        return (stage.at[c], out), pl.ds(pl.multiple_of((me * chunks + c) * width, width), width), c + 1

    def to_own(c, m):
        (source, out), columns, s = place(c, m)
        return pltpu.make_async_copy(source.at[pl.ds(pl.multiple_of(me * height, height), height)], out.at[:, columns], kept.at[s, m])

    def to_peer(c, m, j):
        (source, out), columns, s = place(c, m)
        peer = lax.rem(me + j, GROUP)
        return pltpu.make_async_remote_copy(
            src_ref=source.at[pl.ds(pl.multiple_of(peer * height, height), height)], dst_ref=out.at[:, columns],
            send_sem=sends.at[s, m, j - 1], recv_sem=receives.at[s, m, j - 1], device_id=(rep, peer), device_id_type=pl.DeviceIdType.MESH)

    def spread(c, m):
        for j in (4, 3, 5, 2, 6, 1, 7):
            to_peer(c, m, j).start()
        to_own(c, m).start()

    @pl.when((chunk == 0) & (step == 1))
    def _():
        pl.semaphore_wait(barrier, GROUP - 1)
        for m in range(2):
            spread(-1, m)

    @pl.when(step == steps - 1)
    def _():
        for m, stage, acc in ((0, stageg_ref, accg_ref), (1, stageu_ref, accu_ref)):
            stage[chunk] = acc[...].astype(BF16)
            spread(chunk, m)
        bd_ref[...] = accd_ref[...].astype(BF16)

    @pl.when((chunk == chunks - 1) & (step == steps - 1))
    def _():
        for m in range(2):
            to_own(-1, m).wait()
            for j in range(1, GROUP):
                to_peer(-1, m, j).wait()

        def finish(c, _):
            for m in range(2):
                to_own(c, m).wait()
                for j in range(1, GROUP):
                    to_peer(c, m, j).wait()
            return 0

        lax.fori_loop(0, chunks, finish, 0)


def weights_back(a, g, wg, wu, wd, layer, ready=None, width=256, block=1024):
    tokens, d = a.shape
    ff = wd.shape[1]
    chunks = ff // width
    rows = pl.BlockSpec((block, d), lambda k, t: (t, 0))
    column = pl.BlockSpec((d, width), lambda k, t: (0, lax.axis_index("dp") * chunks + k))
    column_out = pl.BlockSpec((d, width), lambda k, t: (0, k))
    down = pl.BlockSpec((None, width, d), lambda k, t: (layer, k, 0))
    down_out = pl.BlockSpec((width, d), lambda k, t: (k, 0))
    anywhere = pl.BlockSpec(memory_space=pltpu.HBM)
    accs = [pltpu.VMEM((d, width), F32), pltpu.VMEM((d, width), F32), pltpu.VMEM((width, d), F32)]
    half = jax.ShapeDtypeStruct((d, ff), BF16)
    bd = jax.ShapeDtypeStruct((ff, d), BF16)
    cost = pl.CostEstimate(flops=12 * tokens * d * ff, bytes_accessed=4 * d * tokens * chunks, transcendentals=tokens * ff)
    common = dict(grid=(chunks, tokens // block), cost_estimate=cost)
    if ready is None:
        return pl.pallas_call(
            upper_kernel, in_specs=[rows, rows, column, column, down], out_specs=[column_out, column_out, down_out],
            out_shape=[half, half, bd], scratch_shapes=accs, name="weights_upper", **common)(a, g, wg, wu, wd)
    spread = jax.ShapeDtypeStruct((d // GROUP, ff * GROUP), BF16)
    dma = pltpu.SemaphoreType.DMA
    return pl.pallas_call(
        lower_kernel,
        in_specs=[rows, rows, column, column, down, anywhere, anywhere],
        out_specs=[anywhere, anywhere, down_out, anywhere, anywhere],
        out_shape=[spread, spread, bd, spread, spread],
        scratch_shapes=accs + [pltpu.VMEM((chunks, d, width), BF16), pltpu.VMEM((chunks, d, width), BF16), dma((chunks + 1, 2)),
                               dma((chunks + 1, 2, GROUP - 1)), dma((chunks + 1, 2, GROUP - 1))],
        compiler_params=pltpu.CompilerParams(collective_id=2, has_side_effects=True), name="weights_lower", **common,
    )(a, g, wg, wu, wd, *ready)


MESH = pl.DeviceIdType.MESH


class Gather:
    def __init__(self, n, own, out, stage, load, store, zs, zr, hs, ps, pr, fs, fr, cs, cr):
        self.n, self.own, self.out, self.stage = n, own, out, stage
        self.load, self.store = load, store
        self.zs, self.zr, self.hs, self.ps, self.pr, self.fs, self.fr, self.cs, self.cr = zs, zr, hs, ps, pr, fs, fr, cs, cr
        rep, dp = lax.axis_index("rep"), lax.axis_index("dp")
        z, core = dp // 2, lax.rem(dp, 2)
        self.rep, self.dp, self.z, self.core = rep, dp, z, core
        self.inner = lax.rem((z + 1) // 2, 2)
        self.high = z // 2
        self.over_x = lax.rem(rep + 2, 4)
        self.over_y = rep + 1 - 2 * lax.rem(rep, 2)
        self.across = 3 - rep
        self.to_x, self.to_y, self.to_core = (self.over_x, dp), (self.over_y, dp), (rep, z * 2 + 1 - core)
        self.sent, self.handed = [], []

    def along(self, z):
        return (self.rep, z * 2 + self.core)

    def source(self, k):
        low = (1 - self.z, 2, 3)[k]
        high = (5 - self.z, 1, 0)[k]
        return self.high * high + (1 - self.high) * low

    def barrier(self):
        semaphore = pltpu.get_barrier_semaphore()
        peers = [self.along(lax.rem(self.z + j, 4)) for j in (1, 2, 3)] + [self.to_x, self.to_y, self.to_core]
        for peer in peers:
            pl.semaphore_signal(semaphore, inc=1, device_id=peer, device_id_type=MESH)
        pl.semaphore_wait(semaphore, len(peers))

    def rows(self, i, z, core, quarter=None):
        size = self.own[i].shape[0]
        start = (z * 2 + core) * size
        if quarter is None:
            return self.out[i].at[pl.ds(pl.multiple_of(start, size), size)]
        part = size // 4
        return self.out[i].at[pl.ds(pl.multiple_of(start + quarter * part, part), part)]

    def copy(self, src, dst, send, receive, peer):
        return pltpu.make_async_remote_copy(src_ref=src, dst_ref=dst, send_sem=send, recv_sem=receive, device_id=peer, device_id_type=MESH)

    def start(self, *args):
        copy = self.copy(*args)
        copy.start()
        self.sent.append(copy)

    def begin(self, i):
        part = self.own[i].shape[0] // 4
        mine = self.own[i].at[pl.ds(pl.multiple_of(self.rep * part, part), part)]
        there = self.rows(i, self.z, self.core, self.rep)
        inner = self.inner
        outward = inner * (3 * self.z - 3) + (1 - inner) * (2 - self.z // 3)
        self.start(mine, there, self.zs.at[2 * i], self.zr.at[3 * i + inner], self.along(1 + lax.rem(self.z, 2)))
        self.start(mine, there, self.zs.at[2 * i + 1], self.zr.at[3 * i + 2 * (1 - inner)], self.along(outward))
        self.start(self.own[i], self.rows(i, self.z, self.core), self.cs.at[4 * i], self.cr.at[4 * i], self.to_core)
        self.local(i, 0).start()

    def local(self, i, leg):
        if leg == 0:
            return pltpu.make_async_copy(self.own[i], self.stage[i], self.load.at[i])
        return pltpu.make_async_copy(self.stage[i], self.rows(i, self.z, self.core), self.store.at[i])

    def keep(self, i):
        self.local(i, 0).wait()
        self.local(i, 1).start()

    def arrived(self, i, k, quarter, semaphore):
        ref = self.rows(i, self.source(k), self.core, quarter)
        self.copy(ref, ref, self.ps.at[0], semaphore, self.to_x).wait_recv()
        return ref

    def plane(self, i, k):
        at = 3 * i + k
        ref = self.arrived(i, k, self.rep, self.zr.at[at])
        if k:
            hand = self.copy(ref, ref, self.hs.at[2 * i + k - 1], self.zr.at[at], self.along(3 * self.high))
            pl.when(self.inner == 1)(hand.start)
            self.handed.append(hand)
        self.start(ref, ref, self.ps.at[2 * at], self.pr.at[2 * at], self.to_x)
        self.start(ref, ref, self.ps.at[2 * at + 1], self.pr.at[2 * at + 1], self.to_y)

    def diagonal(self, i, k):
        at = 3 * i + k
        from_x = self.arrived(i, k, self.over_x, self.pr.at[2 * at])
        from_y = self.arrived(i, k, self.over_y, self.pr.at[2 * at + 1])
        if at % 2:
            self.start(from_x, from_x, self.fs.at[at], self.fr.at[at], self.to_y)
        else:
            self.start(from_y, from_y, self.fs.at[at], self.fr.at[at], self.to_x)

    def share(self, i, k):
        self.arrived(i, k, self.across, self.fr.at[3 * i + k])
        ref = self.rows(i, self.source(k), self.core)
        self.start(ref, ref, self.cs.at[4 * i + k + 1], self.cr.at[4 * i + k + 1], self.to_core)

    def shared(self, i):
        for k in range(4):
            ref = self.rows(i, self.source(k - 1) if k else self.z, 1 - self.core)
            self.copy(ref, ref, self.ps.at[0], self.cr.at[4 * i + k], self.to_core).wait_recv()
        self.local(i, 1).wait()

    def steps(self, lag=2):
        items = [(i, k) for i in range(self.n) for k in range(3)]
        for step in range(len(items) + 2 * lag):
            if step < len(items):
                self.plane(*items[step])
            if lag <= step < len(items) + lag:
                self.diagonal(*items[step - lag])
            if 2 * lag <= step:
                self.share(*items[step - 2 * lag])
            yield step

    def finish(self):
        for copy in self.sent:
            copy.wait_send()
        for hand in self.handed:
            pl.when(self.inner == 1)(hand.wait_send)

    @staticmethod
    def scratch(blocks):
        n, dma = len(blocks), pltpu.SemaphoreType.DMA
        sizes = (n, n, 2 * n, 3 * n, 2 * n, 6 * n, 6 * n, 3 * n, 3 * n, 4 * n, 4 * n)
        return [pltpu.VMEM(b.shape, b.dtype) for b in blocks] + [dma((s,)) for s in sizes]


WIDTH = 512
FIRST_STEP = 14


def gather_kernel(h_ref, wg_ref, wu_ref, wd_ref, *refs):
    n = 6
    out, (h1_ref, a1_ref) = refs[:n], refs[n:n + 2]
    a_ref, acc_ref, wgb, wub, wdb, fetched = refs[n + 2:n + 8]
    scratch = refs[n + 8:]
    g = Gather(n, [w.at[layer] for layer in range(2) for w in (wg_ref, wu_ref, wd_ref)], out, scratch[:n], *scratch[n:])
    g.barrier()
    for i in range(n):
        g.begin(i)
    for i in range(n):
        g.keep(i)
    a_ref[...] = normed(h_ref[...])
    acc_ref[...] = jnp.zeros_like(acc_ref)
    chunks = out[2].shape[0] // WIDTH

    def fetch(c, slot):
        units = pl.ds(pl.multiple_of(c * WIDTH, WIDTH), WIDTH)
        return (pltpu.make_async_copy(out[0].at[:, units], wgb.at[slot], fetched.at[0, slot]),
                pltpu.make_async_copy(out[1].at[:, units], wub.at[slot], fetched.at[1, slot]),
                pltpu.make_async_copy(out[2].at[units], wdb.at[slot], fetched.at[2, slot]))

    def chunk(c, _):
        slot = lax.rem(c, 2)

        @pl.when(c + 1 < chunks)
        def _():
            for copy in fetch(c + 1, 1 - slot):
                copy.start()

        for copy in fetch(c, slot):
            copy.wait()
        for r in range(0, h_ref.shape[0], ROWS):
            rows = pl.ds(r, ROWS)
            a = a_ref[rows, :]
            gate, up = dot(a, wgb[slot], 1, 0), dot(a, wub[slot], 1, 0)
            p = (gate * jax.nn.sigmoid(gate) * up).astype(BF16)
            acc_ref[rows, :] += dot(p, wdb[slot], 1, 0)
        return 0

    for step in g.steps():
        turn, off = divmod(step - FIRST_STEP, 2)
        if turn < 0 or off:
            continue
        if turn == 0:
            for i in range(3):
                g.shared(i)
            for copy in fetch(0, 0):
                copy.start()
        lax.fori_loop(turn * chunks // 4, (turn + 1) * chunks // 4, chunk, 0)
    h = h_ref[...] + acc_ref[...].astype(BF16)
    h1_ref[...] = h
    a1_ref[...] = normed(h)
    for i in range(3, n):
        g.shared(i)
    g.finish()


def gather(h, wg, wu, wd):
    blocks = [jax.ShapeDtypeStruct(w.shape[1:], w.dtype) for _ in range(2) for w in (wg, wu, wd)]
    anywhere = pl.BlockSpec(memory_space=pltpu.HBM)
    vmem = pl.BlockSpec(memory_space=pltpu.VMEM)
    tokens, d = h.shape
    return pl.pallas_call(
        gather_kernel,
        in_specs=[vmem] + [anywhere] * 3,
        out_specs=[anywhere] * 6 + [vmem] * 2,
        out_shape=[jax.ShapeDtypeStruct((8 * b.shape[0], b.shape[1]), b.dtype) for b in blocks] + [jax.ShapeDtypeStruct(h.shape, BF16)] * 2,
        scratch_shapes=[pltpu.VMEM((tokens, d), BF16), pltpu.VMEM((tokens, d), F32), pltpu.VMEM((2, d, WIDTH), BF16),
                        pltpu.VMEM((2, d, WIDTH), BF16), pltpu.VMEM((2, WIDTH, d), BF16), pltpu.SemaphoreType.DMA((3, 2))]
        + Gather.scratch(blocks),
        compiler_params=pltpu.CompilerParams(collective_id=0, has_side_effects=True),
        cost_estimate=pl.CostEstimate(flops=200_000_000_000, bytes_accessed=48 * 2**20, transcendentals=0),
        name="gather",
    )(h, wg, wu, wd)


def solution(mesh):
    def body(x, dy, wg, wu, wd):
        gather_all = functools.partial(lax.all_gather, axis_name="dp", axis=0, tiled=True)
        h0, g2 = x[0], dy[0]
        all_g2, all_a0 = gather_all(g2), gather_all(normed(h0))
        *flat, h1, a1 = gather(h0, wg, wu, wd)
        lower, upper = flat[:3], flat[3:]
        h1, all_g2, all_a0 = lax.optimization_barrier((h1, all_g2, all_a0))
        all_a1 = gather_all(a1)
        g1 = back(h1, g2, *upper)
        all_g1 = gather_all(g1)
        g0 = back(h0, g1, *lower)
        all_a1, g0 = lax.optimization_barrier((all_a1, g0))
        bg1, bu1, bd1 = weights_back(all_a1, all_g2, *upper[:2], wd, 1, width=512)
        all_g1, bg1, bu1, bd1 = lax.optimization_barrier((all_g1, bg1, bu1, bd1))
        bg0, bu0, bd0, bg1, bu1 = weights_back(all_a0, all_g1, *lower[:2], wd, 0, ready=(bg1, bu1))
        return (g0[None], *(jnp.stack(t) for t in ((bg0, bg1), (bu0, bu1), (bd0, bd1))))

    rows = P(("rep", "dp"), None, None)
    w = P(None, "dp", None)
    out = P("rep", "dp", None)
    return jax.shard_map(body, mesh=mesh, in_specs=(rows, rows, w, w, w), out_specs=(rows, out, out, out), check_vma=False)
```

```python
import functools

import jax
import jax.numpy as jnp
from jax import lax
from jax.experimental import pallas as pl
from jax.experimental.pallas import tpu as pltpu
from jax.sharding import PartitionSpec as P

F32, BF16 = jnp.float32, jnp.bfloat16


def normed(h):
    wide = h.astype(F32)
    scale = lax.rsqrt(jnp.mean(wide**2, -1, keepdims=True) + 1e-6)
    return (wide * scale).astype(BF16)


def dot(a, b, ca, cb):
    return lax.dot_general(a, b, (((ca,), (cb,)), ((), ())), preferred_element_type=F32)


def norm_back(h, da):
    wide = h.astype(F32)
    scale = lax.rsqrt(jnp.mean(wide**2, -1, keepdims=True) + 1e-6)
    da = da.astype(F32)
    inner = jnp.sum(da * wide, -1, keepdims=True)
    return (da * scale - wide * (scale**3 * inner / h.shape[-1])).astype(BF16)


def hidden_back(gate, up, dp):
    dp = dp.astype(BF16).astype(F32)
    sig = jax.nn.sigmoid(gate)
    s = gate * sig
    return (s * up).astype(BF16), (dp * up * (sig + s * (1 - sig))).astype(BF16), (dp * s).astype(BF16)


ROWS = 512


def back_kernel(h_ref, g_ref, wg_ref, wu_ref, wd_ref, out_ref, a_ref, accg_ref, accu_ref):
    step = pl.program_id(0)

    @pl.when(step == 0)
    def _():
        a_ref[...] = normed(h_ref[...])
        accg_ref[...] = jnp.zeros_like(accg_ref)
        accu_ref[...] = jnp.zeros_like(accu_ref)

    for r in range(0, h_ref.shape[0], ROWS):
        rows = pl.ds(r, ROWS)
        a = a_ref[rows, :]
        gate, up = dot(a, wg_ref[...], 1, 0), dot(a, wu_ref[...], 1, 0)
        _, dgate, dup = hidden_back(gate, up, dot(g_ref[rows, :], wd_ref[...], 1, 1))
        accg_ref[rows, :] += dot(dgate, wg_ref[...], 1, 1)
        accu_ref[rows, :] += dot(dup, wu_ref[...], 1, 1)

    @pl.when(step == pl.num_programs(0) - 1)
    def _():
        da = accg_ref[...].astype(BF16) + accu_ref[...].astype(BF16)
        out_ref[...] = g_ref[...] + norm_back(h_ref[...], da)


def back(h, g, wg, wu, wd, width=1024):
    tokens, d = h.shape
    ff = wd.shape[0]
    whole = pl.BlockSpec((tokens, d), lambda k: (0, 0))
    column = pl.BlockSpec((d, width), lambda k: (0, k))
    return pl.pallas_call(
        back_kernel,
        grid=(ff // width,),
        in_specs=[whole, whole, column, column, pl.BlockSpec((width, d), lambda k: (k, 0))],
        out_specs=whole,
        out_shape=jax.ShapeDtypeStruct(h.shape, BF16),
        scratch_shapes=[pltpu.VMEM((tokens, d), BF16), pltpu.VMEM((tokens, d), F32), pltpu.VMEM((tokens, d), F32)],
        cost_estimate=pl.CostEstimate(flops=10 * tokens * d * ff, bytes_accessed=6 * d * ff, transcendentals=tokens * ff),
        name="back",
    )(h, g, wg, wu, wd)


GROUP = 8


def weights_step(a_ref, g_ref, wg_ref, wu_ref, wd_ref, accg_ref, accu_ref, accd_ref):
    @pl.when(pl.program_id(1) == 0)
    def _():
        for acc in (accg_ref, accu_ref, accd_ref):
            acc[...] = jnp.zeros_like(acc)

    ps, dgs, dus = [], [], []
    for r in range(0, a_ref.shape[0], ROWS):
        rows = pl.ds(r, ROWS)
        a, g = a_ref[rows, :], g_ref[rows, :]
        gate, up = dot(a, wg_ref[...], 1, 0), dot(a, wu_ref[...], 1, 0)
        p, dgate, dup = hidden_back(gate, up, dot(g, wd_ref[...], 1, 1))
        ps.append(p), dgs.append(dgate), dus.append(dup)
    p, dgate, dup = (jnp.concatenate(t, 0) for t in (ps, dgs, dus))
    accg_ref[...] += dot(a_ref[...], dgate, 0, 0)
    accu_ref[...] += dot(a_ref[...], dup, 0, 0)
    accd_ref[...] += dot(p, g_ref[...], 0, 0)


def upper_kernel(a_ref, g_ref, wg_ref, wu_ref, wd_ref, bg_ref, bu_ref, bd_ref, *accs):
    weights_step(a_ref, g_ref, wg_ref, wu_ref, wd_ref, *accs)

    @pl.when(pl.program_id(1) == pl.num_programs(1) - 1)
    def _():
        for out, acc in zip((bg_ref, bu_ref, bd_ref), accs):
            out[...] = acc[...].astype(BF16)


def lower_kernel(a_ref, g_ref, wg_ref, wu_ref, wd_ref, ready_g, ready_u, bg_ref, bu_ref, bd_ref, cg_ref, cu_ref,
                 accg_ref, accu_ref, accd_ref, stageg_ref, stageu_ref, kept, sends, receives):
    chunk, step = pl.program_id(0), pl.program_id(1)
    chunks, steps = pl.num_programs(0), pl.num_programs(1)
    width = wg_ref.shape[1]
    height = bg_ref.shape[0]
    rep, me = lax.axis_index("rep"), lax.axis_index("dp")
    barrier = pltpu.get_barrier_semaphore()

    @pl.when((chunk == 0) & (step == 0))
    def _():
        for j in range(1, GROUP):
            pl.semaphore_signal(barrier, inc=1, device_id=(rep, lax.rem(me + j, GROUP)), device_id_type=pl.DeviceIdType.MESH)

    weights_step(a_ref, g_ref, wg_ref, wu_ref, wd_ref, accg_ref, accu_ref, accd_ref)

    def place(c, m):
        if isinstance(c, int) and c < 0:
            return ((ready_g, cg_ref), (ready_u, cu_ref))[m], pl.ds(pl.multiple_of(me * chunks * width, chunks * width), chunks * width), 0
        stage, out = ((stageg_ref, bg_ref), (stageu_ref, bu_ref))[m]
        return (stage.at[c], out), pl.ds(pl.multiple_of((me * chunks + c) * width, width), width), c + 1

    def to_own(c, m):
        (source, out), columns, s = place(c, m)
        return pltpu.make_async_copy(source.at[pl.ds(pl.multiple_of(me * height, height), height)], out.at[:, columns], kept.at[s, m])

    def to_peer(c, m, j):
        (source, out), columns, s = place(c, m)
        peer = lax.rem(me + j, GROUP)
        return pltpu.make_async_remote_copy(
            src_ref=source.at[pl.ds(pl.multiple_of(peer * height, height), height)], dst_ref=out.at[:, columns],
            send_sem=sends.at[s, m, j - 1], recv_sem=receives.at[s, m, j - 1], device_id=(rep, peer), device_id_type=pl.DeviceIdType.MESH)

    def spread(c, m):
        for j in (4, 3, 5, 2, 6, 1, 7):
            to_peer(c, m, j).start()
        to_own(c, m).start()

    @pl.when((chunk == 0) & (step == 1))
    def _():
        pl.semaphore_wait(barrier, GROUP - 1)
        for m in range(2):
            spread(-1, m)

    @pl.when(step == steps - 1)
    def _():
        for m, stage, acc in ((0, stageg_ref, accg_ref), (1, stageu_ref, accu_ref)):
            stage[chunk] = acc[...].astype(BF16)
            spread(chunk, m)
        bd_ref[...] = accd_ref[...].astype(BF16)

    @pl.when((chunk == chunks - 1) & (step == steps - 1))
    def _():
        for m in range(2):
            to_own(-1, m).wait()
            for j in range(1, GROUP):
                to_peer(-1, m, j).wait()

        def finish(c, _):
            for m in range(2):
                to_own(c, m).wait()
                for j in range(1, GROUP):
                    to_peer(c, m, j).wait()
            return 0

        lax.fori_loop(0, chunks, finish, 0)


def weights_back(a, g, wg, wu, wd, layer, ready=None, width=256, block=1024):
    tokens, d = a.shape
    ff = wd.shape[1]
    chunks = ff // width
    rows = pl.BlockSpec((block, d), lambda k, t: (t, 0))
    column = pl.BlockSpec((d, width), lambda k, t: (0, lax.axis_index("dp") * chunks + k))
    column_out = pl.BlockSpec((d, width), lambda k, t: (0, k))
    down = pl.BlockSpec((None, width, d), lambda k, t: (layer, k, 0))
    down_out = pl.BlockSpec((width, d), lambda k, t: (k, 0))
    anywhere = pl.BlockSpec(memory_space=pltpu.HBM)
    accs = [pltpu.VMEM((d, width), F32), pltpu.VMEM((d, width), F32), pltpu.VMEM((width, d), F32)]
    half = jax.ShapeDtypeStruct((d, ff), BF16)
    bd = jax.ShapeDtypeStruct((ff, d), BF16)
    cost = pl.CostEstimate(flops=12 * tokens * d * ff, bytes_accessed=4 * d * tokens * chunks, transcendentals=tokens * ff)
    common = dict(grid=(chunks, tokens // block), cost_estimate=cost)
    if ready is None:
        return pl.pallas_call(
            upper_kernel, in_specs=[rows, rows, column, column, down], out_specs=[column_out, column_out, down_out],
            out_shape=[half, half, bd], scratch_shapes=accs, name="weights_upper", **common)(a, g, wg, wu, wd)
    spread = jax.ShapeDtypeStruct((d // GROUP, ff * GROUP), BF16)
    dma = pltpu.SemaphoreType.DMA
    return pl.pallas_call(
        lower_kernel,
        in_specs=[rows, rows, column, column, down, anywhere, anywhere],
        out_specs=[anywhere, anywhere, down_out, anywhere, anywhere],
        out_shape=[spread, spread, bd, spread, spread],
        scratch_shapes=accs + [pltpu.VMEM((chunks, d, width), BF16), pltpu.VMEM((chunks, d, width), BF16), dma((chunks + 1, 2)),
                               dma((chunks + 1, 2, GROUP - 1)), dma((chunks + 1, 2, GROUP - 1))],
        compiler_params=pltpu.CompilerParams(collective_id=2, has_side_effects=True), name="weights_lower", **common,
    )(a, g, wg, wu, wd, *ready)


MESH = pl.DeviceIdType.MESH


class Gather:
    def __init__(self, n, own, out, stage, load, store, zs, zr, hs, ps, pr, fs, fr, cs, cr):
        self.n, self.own, self.out, self.stage = n, own, out, stage
        self.load, self.store = load, store
        self.zs, self.zr, self.hs, self.ps, self.pr, self.fs, self.fr, self.cs, self.cr = zs, zr, hs, ps, pr, fs, fr, cs, cr
        rep, dp = lax.axis_index("rep"), lax.axis_index("dp")
        z, core = dp // 2, lax.rem(dp, 2)
        self.rep, self.dp, self.z, self.core = rep, dp, z, core
        self.inner = lax.rem((z + 1) // 2, 2)
        self.high = z // 2
        self.over_x = lax.rem(rep + 2, 4)
        self.over_y = rep + 1 - 2 * lax.rem(rep, 2)
        self.across = 3 - rep
        self.to_x, self.to_y, self.to_core = (self.over_x, dp), (self.over_y, dp), (rep, z * 2 + 1 - core)
        self.sent, self.handed = [], []

    def along(self, z):
        return (self.rep, z * 2 + self.core)

    def source(self, k):
        low = (1 - self.z, 2, 3)[k]
        high = (5 - self.z, 1, 0)[k]
        return self.high * high + (1 - self.high) * low

    def barrier(self):
        semaphore = pltpu.get_barrier_semaphore()
        peers = [self.along(lax.rem(self.z + j, 4)) for j in (1, 2, 3)] + [self.to_x, self.to_y, self.to_core]
        for peer in peers:
            pl.semaphore_signal(semaphore, inc=1, device_id=peer, device_id_type=MESH)
        pl.semaphore_wait(semaphore, len(peers))

    def rows(self, i, z, core, quarter=None):
        size = self.own[i].shape[0]
        start = (z * 2 + core) * size
        if quarter is None:
            return self.out[i].at[pl.ds(pl.multiple_of(start, size), size)]
        part = size // 4
        return self.out[i].at[pl.ds(pl.multiple_of(start + quarter * part, part), part)]

    def copy(self, src, dst, send, receive, peer):
        return pltpu.make_async_remote_copy(src_ref=src, dst_ref=dst, send_sem=send, recv_sem=receive, device_id=peer, device_id_type=MESH)

    def start(self, *args):
        copy = self.copy(*args)
        copy.start()
        self.sent.append(copy)

    def begin(self, i):
        part = self.own[i].shape[0] // 4
        mine = self.own[i].at[pl.ds(pl.multiple_of(self.rep * part, part), part)]
        there = self.rows(i, self.z, self.core, self.rep)
        inner = self.inner
        outward = inner * (3 * self.z - 3) + (1 - inner) * (2 - self.z // 3)
        self.start(mine, there, self.zs.at[2 * i], self.zr.at[3 * i + inner], self.along(1 + lax.rem(self.z, 2)))
        self.start(mine, there, self.zs.at[2 * i + 1], self.zr.at[3 * i + 2 * (1 - inner)], self.along(outward))
        self.start(self.own[i], self.rows(i, self.z, self.core), self.cs.at[4 * i], self.cr.at[4 * i], self.to_core)
        self.local(i, 0).start()

    def local(self, i, leg):
        if leg == 0:
            return pltpu.make_async_copy(self.own[i], self.stage[i], self.load.at[i])
        return pltpu.make_async_copy(self.stage[i], self.rows(i, self.z, self.core), self.store.at[i])

    def keep(self, i):
        self.local(i, 0).wait()
        self.local(i, 1).start()

    def arrived(self, i, k, quarter, semaphore):
        ref = self.rows(i, self.source(k), self.core, quarter)
        self.copy(ref, ref, self.ps.at[0], semaphore, self.to_x).wait_recv()
        return ref

    def plane(self, i, k):
        at = 3 * i + k
        ref = self.arrived(i, k, self.rep, self.zr.at[at])
        if k:
            hand = self.copy(ref, ref, self.hs.at[2 * i + k - 1], self.zr.at[at], self.along(3 * self.high))
            pl.when(self.inner == 1)(hand.start)
            self.handed.append(hand)
        self.start(ref, ref, self.ps.at[2 * at], self.pr.at[2 * at], self.to_x)
        self.start(ref, ref, self.ps.at[2 * at + 1], self.pr.at[2 * at + 1], self.to_y)

    def diagonal(self, i, k):
        at = 3 * i + k
        from_x = self.arrived(i, k, self.over_x, self.pr.at[2 * at])
        from_y = self.arrived(i, k, self.over_y, self.pr.at[2 * at + 1])
        if at % 2:
            self.start(from_x, from_x, self.fs.at[at], self.fr.at[at], self.to_y)
        else:
            self.start(from_y, from_y, self.fs.at[at], self.fr.at[at], self.to_x)

    def share(self, i, k):
        self.arrived(i, k, self.across, self.fr.at[3 * i + k])
        ref = self.rows(i, self.source(k), self.core)
        self.start(ref, ref, self.cs.at[4 * i + k + 1], self.cr.at[4 * i + k + 1], self.to_core)

    def shared(self, i):
        for k in range(4):
            ref = self.rows(i, self.source(k - 1) if k else self.z, 1 - self.core)
            self.copy(ref, ref, self.ps.at[0], self.cr.at[4 * i + k], self.to_core).wait_recv()
        self.local(i, 1).wait()

    def steps(self, lag=2):
        items = [(i, k) for i in range(self.n) for k in range(3)]
        for step in range(len(items) + 2 * lag):
            if step < len(items):
                self.plane(*items[step])
            if lag <= step < len(items) + lag:
                self.diagonal(*items[step - lag])
            if 2 * lag <= step:
                self.share(*items[step - 2 * lag])
            yield step

    def finish(self):
        for copy in self.sent:
            copy.wait_send()
        for hand in self.handed:
            pl.when(self.inner == 1)(hand.wait_send)

    @staticmethod
    def scratch(blocks):
        n, dma = len(blocks), pltpu.SemaphoreType.DMA
        sizes = (n, n, 2 * n, 3 * n, 2 * n, 6 * n, 6 * n, 3 * n, 3 * n, 4 * n, 4 * n)
        return [pltpu.VMEM(b.shape, b.dtype) for b in blocks] + [dma((s,)) for s in sizes]


class Line:
    PARTS = 2

    def __init__(self, g, own, out, kept, zs, zr, hs, cs, cr):
        self.g, self.own, self.out, self.kept = g, own, out, kept
        self.zs, self.zr, self.hs, self.cs, self.cr = zs, zr, hs, cs, cr
        self.size = own.shape[0] // self.PARTS

    def piece(self, z, core, part):
        return self.out.at[pl.ds(pl.multiple_of((z * 2 + core) * self.own.shape[0] + part * self.size, self.size), self.size)]

    def local(self, part):
        g = self.g
        return pltpu.make_async_copy(self.own.at[pl.ds(part * self.size, self.size)], self.piece(g.z, g.core, part), self.kept.at[part])

    def begin(self):
        g = self.g
        outward = g.inner * (3 * g.z - 3) + (1 - g.inner) * (2 - g.z // 3)
        for part in range(self.PARTS):
            mine, there = self.own.at[pl.ds(part * self.size, self.size)], self.piece(g.z, g.core, part)
            g.start(mine, there, self.zs.at[part, 0], self.zr.at[part, g.inner], g.along(1 + lax.rem(g.z, 2)))
            g.start(mine, there, self.zs.at[part, 1], self.zr.at[part, 2 * (1 - g.inner)], g.along(outward))
            g.start(mine, there, self.cs.at[part, 3], self.cr.at[part, 3], g.to_core)
            self.local(part).start()

    def step(self, part, k):
        g = self.g
        ref = self.piece(g.source(k), g.core, part)
        g.copy(ref, ref, self.zs.at[part, 0], self.zr.at[part, k], g.to_core).wait_recv()
        if k:
            hand = g.copy(ref, ref, self.hs.at[part, k - 1], self.zr.at[part, k], g.along(3 * g.high))
            pl.when(g.inner == 1)(hand.start)
            g.handed.append(hand)
        g.start(ref, ref, self.cs.at[part, k], self.cr.at[part, k], g.to_core)

    def steps(self):
        return [(self, part, k) for part in range(self.PARTS) for k in range(3)]

    def finish(self):
        g = self.g
        for part in range(self.PARTS):
            for k in range(4):
                ref = self.piece(g.source(k) if k < 3 else g.z, 1 - g.core, part)
                g.copy(ref, ref, self.zs.at[part, 0], self.cr.at[part, k], g.to_core).wait_recv()
            self.local(part).wait()

    @classmethod
    def scratch(cls):
        return [pltpu.SemaphoreType.DMA(s) for s in ((cls.PARTS,), (cls.PARTS, 2), (cls.PARTS, 3), (cls.PARTS, 2), (cls.PARTS, 4), (cls.PARTS, 4))]


WIDTH = 512
TURNS = (14, 16, 18, 20)
FIRST_LINE_STEP = 10


def gather_kernel(h_ref, g_ref, wg_ref, wu_ref, wd_ref, *refs):
    n = 6
    out, (h1_ref, a1_ref, allg_ref, alla_ref) = refs[:n], refs[n:n + 4]
    a0_ref, acc_ref, wgb, wub, wdb, fetched = refs[n + 4:n + 10]
    lines, scratch = refs[n + 10:n + 22], refs[n + 22:]
    g = Gather(n, [w.at[layer] for layer in range(2) for w in (wg_ref, wu_ref, wd_ref)], out, scratch[:n], *scratch[n:])
    lines = [Line(g, g_ref, allg_ref, *lines[:6]), Line(g, a0_ref, alla_ref, *lines[6:])]
    a0_ref[...] = normed(h_ref[...])
    g.barrier()
    for i in range(n):
        g.begin(i)
    for line in lines:
        line.begin()
    for i in range(n):
        g.keep(i)
    acc_ref[...] = jnp.zeros_like(acc_ref)
    chunks = out[2].shape[0] // WIDTH

    def fetch(c, slot):
        units = pl.ds(pl.multiple_of(c * WIDTH, WIDTH), WIDTH)
        return (pltpu.make_async_copy(out[0].at[:, units], wgb.at[slot], fetched.at[0, slot]),
                pltpu.make_async_copy(out[1].at[:, units], wub.at[slot], fetched.at[1, slot]),
                pltpu.make_async_copy(out[2].at[units], wdb.at[slot], fetched.at[2, slot]))

    def chunk(c, _):
        slot = lax.rem(c, 2)

        @pl.when(c + 1 < chunks)
        def _():
            for copy in fetch(c + 1, 1 - slot):
                copy.start()

        for copy in fetch(c, slot):
            copy.wait()
        for r in range(0, h_ref.shape[0], ROWS):
            rows = pl.ds(r, ROWS)
            a = a0_ref[rows, :]
            gate, up = dot(a, wgb[slot], 1, 0), dot(a, wub[slot], 1, 0)
            p = (gate * jax.nn.sigmoid(gate) * up).astype(BF16)
            acc_ref[rows, :] += dot(p, wdb[slot], 1, 0)
        return 0

    waiting = [step for line in lines for step in line.steps()]
    for step in g.steps():
        if step in TURNS:
            turn = TURNS.index(step)
            if turn == 0:
                for i in range(3):
                    g.shared(i)
                for copy in fetch(0, 0):
                    copy.start()
            lax.fori_loop(turn * chunks // len(TURNS), (turn + 1) * chunks // len(TURNS), chunk, 0)
        if step >= FIRST_LINE_STEP and waiting:
            line, part, k = waiting.pop(0)
            line.step(part, k)
    h = h_ref[...] + acc_ref[...].astype(BF16)
    h1_ref[...] = h
    a1_ref[...] = normed(h)
    for i in range(3, n):
        g.shared(i)
    for line in lines:
        line.finish()
    g.finish()


def gather(h, dy, wg, wu, wd):
    blocks = [jax.ShapeDtypeStruct(w.shape[1:], w.dtype) for _ in range(2) for w in (wg, wu, wd)]
    anywhere = pl.BlockSpec(memory_space=pltpu.HBM)
    vmem = pl.BlockSpec(memory_space=pltpu.VMEM)
    tokens, d = h.shape
    return pl.pallas_call(
        gather_kernel,
        in_specs=[vmem] * 2 + [anywhere] * 3,
        out_specs=[anywhere] * 6 + [vmem] * 2 + [anywhere] * 2,
        out_shape=[jax.ShapeDtypeStruct((8 * b.shape[0], b.shape[1]), b.dtype) for b in blocks] + [jax.ShapeDtypeStruct(h.shape, BF16)] * 2
        + [jax.ShapeDtypeStruct((8 * tokens, d), BF16)] * 2,
        scratch_shapes=[pltpu.VMEM((tokens, d), BF16), pltpu.VMEM((tokens, d), F32), pltpu.VMEM((2, d, WIDTH), BF16),
                        pltpu.VMEM((2, d, WIDTH), BF16), pltpu.VMEM((2, WIDTH, d), BF16), pltpu.SemaphoreType.DMA((3, 2))]
        + Line.scratch() + Line.scratch() + Gather.scratch(blocks),
        compiler_params=pltpu.CompilerParams(collective_id=0, has_side_effects=True),
        cost_estimate=pl.CostEstimate(flops=200_000_000_000, bytes_accessed=48 * 2**20, transcendentals=0),
        name="gather",
    )(h, dy, wg, wu, wd)


def solution(mesh):
    def body(x, dy, wg, wu, wd):
        gather_all = functools.partial(lax.all_gather, axis_name="dp", axis=0, tiled=True)
        h0, g2 = x[0], dy[0]
        *flat, h1, a1, all_g2, all_a0 = gather(h0, g2, wg, wu, wd)
        lower, upper = flat[:3], flat[3:]
        all_a1 = gather_all(a1)
        g1 = back(h1, g2, *upper)
        all_g1 = gather_all(g1)
        g0 = back(h0, g1, *lower)
        all_a1, g0 = lax.optimization_barrier((all_a1, g0))
        bg1, bu1, bd1 = weights_back(all_a1, all_g2, *upper[:2], wd, 1, width=512)
        all_g1, bg1, bu1, bd1 = lax.optimization_barrier((all_g1, bg1, bu1, bd1))
        bg0, bu0, bd0, bg1, bu1 = weights_back(all_a0, all_g1, *lower[:2], wd, 0, ready=(bg1, bu1))
        return (g0[None], *(jnp.stack(t) for t in ((bg0, bg1), (bu0, bu1), (bd0, bd1))))

    rows = P(("rep", "dp"), None, None)
    w = P(None, "dp", None)
    out = P("rep", "dp", None)
    return jax.shard_map(body, mesh=mesh, in_specs=(rows, rows, w, w, w), out_specs=(rows, out, out, out), check_vma=False)
```
